32 devices in a mesh: expert: 4 (over x, core), ffn: 8 (over z, y).
Axes of the slice: x: 2, y: 2, z: 4, core: 2. Of those that a mesh axis runs over, the one named last changes fastest.
Arguments:
- tokens: bfloat16 [4, 32, 4096], P('expert', 'ffn'), may hold values from -6 to 6
- routes: int32 [4, 32, 2], P('expert'), may hold values from 0 to 3, all different within a row; in each aligned block of 32 rows (0 to 31, 32 to 63, ..., all dimensions but the last counted through in order) at most 24 rows name the same one
- router: bfloat16 [4096, 4], replicated, may hold values from -0.09375 to 0.09375
- w_gate: bfloat16 [4, 4096, 12288], P('expert', None, 'ffn'), may hold values from -0.09375 to 0.09375
- w_up: bfloat16 [4, 4096, 12288], P('expert', None, 'ffn'), may hold values from -0.09375 to 0.09375
- w_down: bfloat16 [4, 12288, 4096], P('expert', 'ffn'), may hold values from -0.078125 to 0.078125
- adapter: bfloat16 [4, 4096, 4096], P('expert', None, 'ffn'), may hold values from -0.09375 to 0.09375
- upstream: bfloat16 [4, 32, 4096], P('expert', None, 'ffn'), may hold values from -24 to 24
- bound: float32 [4], P('expert'), may hold values from 2048 to 16384
Outputs:
- adapted: bfloat16 [4, 32, 4096], P('expert', None, 'ffn')
- clipped: bfloat16 [4, 4096, 4096], P('expert', None, 'ffn')
The draws below stay inside these ranges and needn't reach their ends.
Inputs may be any that keep to these rules, and one draw needn't show every extreme that they name: `routes`: each token names two different experts; for each client at most 24 of its tokens name any one expert, and in some clients some expert is named by exactly 24 tokens.
All inputs are finite; a program needn't handle non-finite values.
Results may differ from the reference program's by a relative error of at most 0.015.
Values may be sent and summed in bfloat16 or wider, within the bound.
A program may use at most 128 MiB of HBM per device.

```python
import math
import jax
import jax.numpy as jnp
import numpy as np
from jax import lax

D = 4096
FF = 12288
EXPERTS = 4
CLIENTS = 4
TOK_CL = 32
CAP = 24
FF_DEV = 1536
COLS_DEV = 512
N_FFN = 8


def draw_upstream(key, part):
    key_noise = jax.random.fold_in(key, 11)
    key_scale = jax.random.fold_in(key, 23)
    noise_part = jax.random.normal(key_noise, (CLIENTS, TOK_CL, D), jnp.float32)
    block_scales = jnp.exp(jax.random.uniform(key_scale, (CLIENTS, 1, D // COLS_DEV), jnp.float32, math.log(0.25), math.log(4.0)))
    scales = jnp.repeat(block_scales, COLS_DEV, axis=2)
    values = noise_part * scales
    return jnp.clip(values, -24.0, 24.0).astype(jnp.bfloat16)


def raised(array, own_key, source, target, blocks, factor):
    def block_of(position):
        return (jnp.arange(array.shape[position]) // (array.shape[position] // blocks)).reshape((-1,) + (1,) * (array.ndim - 1 - position))

    first = jax.random.permutation(own_key, blocks)[block_of(target)]
    far = (block_of(target) + blocks // 2) % blocks
    return jnp.where((block_of(source) == first) | (block_of(source) == far), factor * array, array)


def shard_levels(key, extent, cuts, smallest, largest):
    loudness = 1.0
    for position, parts in cuts:
        steps = jax.random.uniform(jax.random.fold_in(jax.random.fold_in(key, 6), position), (parts,), jnp.float32, smallest / len(cuts), largest / len(cuts))
        loudness = loudness * jnp.repeat(jnp.exp(steps), extent[position] // parts).reshape((-1,) + (1,) * (len(extent) - 1 - position))
    return loudness


def routed_block(key, own, number, rows, number_of, top, limit, lean):
    sequence = jax.random.permutation(key, number_of)
    crowded, ordinary = shares(number_of, rows * top, limit, lean, True), shares(number_of, rows * top, limit, lean, False)
    places = jnp.arange(number_of)

    def named(tallies, turn):
        used = int((tallies > 0).sum())
        fixed = max(1, used // 4)
        passed = fixed + (places - fixed + turn * (used - fixed)) % max(1, number_of - fixed)
        return jnp.zeros((number_of,), jnp.int32).at[sequence[jnp.where(places < fixed, places, passed)]].set(jnp.asarray(tallies, jnp.int32))

    tallies = jnp.where(number % 4 == 0, named(crowded, number // 4), named(ordinary, number - number // 4 - 1))
    mixed = jax.random.permutation(jax.random.fold_in(own, 3), number_of)
    donor, taker = mixed[0:number_of // 2 * 2:2], mixed[1:number_of // 2 * 2:2]
    slack = jnp.minimum(tallies[donor] - 1, limit - tallies[taker]) // 2
    slack = jnp.where((donor == sequence[0]) | (taker == sequence[0]) | (tallies[taker] == 0), 0, jnp.maximum(slack, 0))
    passed = jax.random.randint(jax.random.fold_in(own, 4), (number_of // 2,), 0, 1 << 20) % (slack + 1)
    tallies = tallies.at[donor].add(-passed).at[taker].add(passed)
    members = jnp.searchsorted(jnp.cumsum(tallies), jnp.arange(rows * top), side="right").astype(jnp.int32)
    grid = members.reshape(top, rows).T
    grid = grid[jax.random.permutation(jax.random.fold_in(own, 1), rows)]
    turn = jax.random.randint(jax.random.fold_in(own, 2), (rows, 1), 0, top)
    return jnp.take_along_axis(grid, (jnp.arange(top)[None, :] + turn) % top, axis=1)


def shares(amount, total, most, skew, full):
    loads = [(1 << 20) // math.isqrt(grade ** skew) + 1 for grade in range(1, amount + 1)]
    largest = most if full else min(most, max(-(-total // amount), total * loads[0] // sum(loads)))
    least = 1 if total - largest >= amount - 1 else 0
    counts, spare = [largest] + [least] * (amount - 1), total - largest - least * (amount - 1)
    while spare > 0:
        candidates = [i for i in range(1, amount) if counts[i] < largest] or [i for i in range(1, amount) if counts[i] < most]
        pool, left = sum([loads[i] for i in candidates]), spare
        for i in candidates:
            more = min(most - counts[i], max(1, left * loads[i] // pool), spare)
            counts[i] = counts[i] + more
            spare = spare - more
    return np.array(counts)


def noise(key, extent, scale, most, shards=(), held_as=jnp.bfloat16):
    array = jax.random.normal(key, extent, jnp.float32) * scale
    if len(shards) > 0:
        array = shard_levels(key, extent, shards, -0.22, 0.18) * array
    return jnp.clip(array, min=-most, max=most).astype(held_as)


def noise_with(key, dims, scale, limit, pieces, heavy, held_as=jnp.bfloat16):
    array = scale * jax.random.normal(key, dims, jnp.float32)
    if pieces:
        array = array * shard_levels(key, dims, pieces, -0.22, 0.18)
    return jnp.clip(raised(array, jax.random.fold_in(key, 3), *heavy), -limit, limit).astype(held_as)


def setup_inputs(seed: int = 0) -> dict:
    key_list = jax.random.split(jax.random.key(seed), 10)
    tokens = noise(key_list[0], (CLIENTS, TOK_CL, D), 1.0, 6.0, ((0, 4), (1, 8)))
    routes_keys = jax.random.split(jax.random.fold_in(key_list[1], 1), CLIENTS * TOK_CL // TOK_CL)
    routes_turns = jax.random.permutation(jax.random.fold_in(key_list[1], 3), CLIENTS * TOK_CL // TOK_CL)
    routes = jax.vmap(lambda own, number: routed_block(jax.random.fold_in(key_list[1], 2), own, number, TOK_CL, EXPERTS, 2, CAP, 1))(routes_keys, routes_turns).reshape((CLIENTS, TOK_CL, 2))
    router = noise(key_list[2], (D, EXPERTS), D ** -0.5, 0.09375)
    w_gate = noise(key_list[3], (EXPERTS, D, FF), D ** -0.5, 0.09375, ((0, 4), (2, 8)))
    w_up = noise(key_list[4], (EXPERTS, D, FF), D ** -0.5, 0.09375, ((0, 4), (2, 8)))
    w_down = noise_with(key_list[5], (EXPERTS, FF, D), FF ** -0.5, 0.078125, ((0, 4), (1, 8)), (1, 2, 8, 2.0))
    adapter = noise(key_list[6], (CLIENTS, D, D), D ** -0.5, 0.09375, ((0, 4), (2, 8)))
    upstream = draw_upstream(jax.random.fold_in(key_list[9], 71), 0)
    bound = jnp.clip(jnp.exp(math.log(16384.0) - 2.0794415 * jax.random.uniform(key_list[8], (CLIENTS,), jnp.float32) ** shard_levels(key_list[8], (CLIENTS,), ((0, 4),), -0.2, 0.2)), 2048.0, 16384.0)
    return {"tokens": tokens, "routes": routes, "router": router, "w_gate": w_gate, "w_up": w_up, "w_down": w_down, "adapter": adapter, "upstream": upstream, "bound": bound}


def slot_table(routed, expert_count):
    named_hits = lax.optimization_barrier(jnp.sum((routed[:, :, None] == jnp.arange(expert_count, dtype=jnp.int32)[None, None, :]).astype(jnp.int32), axis=1))
    before = jnp.cumsum(named_hits, axis=0) - named_hits
    return jnp.take_along_axis(before, routed, axis=1).astype(jnp.int32)

def pack_rows(token_rows, routed, expert_count, capacity):
    token_count = token_rows.shape[0]
    slot_flat = (routed * capacity + slot_table(routed, expert_count)).astype(jnp.int32)
    owners = jnp.repeat(jnp.arange(token_count, dtype=jnp.int32), 2)
    source = jnp.full((expert_count * capacity,), token_count, jnp.int32).at[slot_flat.reshape(-1)].set(owners)
    padded = jnp.concatenate([token_rows, jnp.zeros((1, token_rows.shape[1]), token_rows.dtype)], axis=0)
    return (padded[source].reshape(expert_count, capacity, token_rows.shape[1]), slot_flat)

def mix_weights(token_rows, routed, router):
    logits = jnp.dot(token_rows, router, preferred_element_type=jnp.float32)
    picked = jnp.take_along_axis(logits, routed, axis=1)
    weight_first = jax.nn.sigmoid(picked[:, 0] - picked[:, 1])
    return (weight_first, 1.0 - weight_first)

def reference(tokens, routes, router, w_gate, w_up, w_down, adapter, upstream, bound):

    def pack_one(token_rows, routed):
        return pack_rows(token_rows, routed, EXPERTS, CAP)
    packed, slot_flats = jax.vmap(pack_one)(tokens, routes)

    def add_block(running, operand_pair):
        down_piece = jnp.dot(operand_pair[0], operand_pair[1], preferred_element_type=jnp.float32).astype(jnp.bfloat16)
        down_piece = lax.optimization_barrier(down_piece)
        return (running + down_piece.astype(jnp.float32), None)

    def expert_one(inputs):
        expert_rows, gate_w, up_w, down_w = inputs
        flat_rows = expert_rows.reshape(-1, D)
        gate_out = jnp.dot(flat_rows, gate_w, preferred_element_type=jnp.float32)
        up_out = jnp.dot(flat_rows, up_w, preferred_element_type=jnp.float32)
        hidden = (jax.nn.silu(gate_out) * up_out).astype(jnp.bfloat16)
        blocks = jnp.transpose(hidden.reshape(-1, N_FFN, FF_DEV), (1, 0, 2))
        down_blocks = down_w.reshape(N_FFN, FF_DEV, D)
        running, _ = lax.scan(add_block, jnp.zeros((CLIENTS * CAP, D), jnp.float32), (blocks, down_blocks))
        return running.reshape(CLIENTS, CAP, D)
    expert_out = lax.map(expert_one, (jnp.moveaxis(packed, 1, 0), w_gate, w_up, w_down))
    by_client = jnp.moveaxis(expert_out, 0, 1).reshape(CLIENTS, EXPERTS * CAP, D)

    def client_one(inputs):
        token_rows, routed, slot_flat, expert_rows, adapt_matrix, grad_input, clip_limit = inputs
        weight_first, weight_second = mix_weights(token_rows, routed, router)
        picked = expert_rows[slot_flat]
        mixture = weight_first[:, None] * picked[:, 0] + weight_second[:, None] * picked[:, 1]
        layer_out = (token_rows.astype(jnp.float32) + mixture).astype(jnp.bfloat16)
        adapted = (layer_out.astype(jnp.float32) + jnp.dot(layer_out, adapt_matrix, preferred_element_type=jnp.float32)).astype(jnp.bfloat16)
        adapter_grad = lax.dot_general(layer_out, grad_input, (((0,), (0,)), ((), ())), preferred_element_type=jnp.float32)
        grad_norm = jnp.sqrt(jnp.sum(adapter_grad * adapter_grad))
        factor = clip_limit / jnp.maximum(grad_norm, clip_limit)
        return (adapted, (adapter_grad * factor).astype(jnp.bfloat16))
    adapted, clipped = lax.map(client_one, (tokens, routes, slot_flats, by_client, adapter, upstream, bound))
    return (adapted, clipped)
```

```python
import functools

import jax
import jax.numpy as jnp
from jax import lax
from jax.experimental import pallas as pl
from jax.experimental.pallas import tpu as pltpu
from jax.sharding import PartitionSpec as P

MESH = pl.DeviceIdType.MESH
CORES = 2


def tile_of(size, choices=(512, 384, 256, 128)):
    for width in choices:
        if size % width == 0:
            return width
    return size


def layer_kernel(
    dims,
    tok_ref, routes_ref, router_ref, wg_hbm, wu_hbm, wd_hbm, ad_hbm, up_ref, bound_ref,
    layer_ref, adapted_ref, factor_ref,
    wg, wu, wd, ad, tokbuf, tokc, gate_acc, up_acc, hid, logit_acc, routes_buf, gram_buf,
    sbuf, r1, s2, r2, s3, r3, lbuf,
    w_sem, own_sem, rt_send, rt_recv, gr_send, gr_recv, tf_send, tf_recv, tx_send, tx_recv,
    tc_send, tc_recv, a_send, a_recv, b_send, b_recv, c_send, c_recv, d_send, d_recv,
):
    E, F, KC, NC, D, FFD, t, tl, cd = dims
    X = E // CORES
    T = E * t
    KW = D // KC
    NW = D // NC
    CW = NW // F
    e = lax.axis_index("expert")
    f = lax.axis_index("ffn")
    x, core = e // CORES, lax.rem(e, CORES)
    mate = x * CORES + (CORES - 1 - core)

    loads = {}
    for k in range(KC):
        loads["g", k] = pltpu.make_async_copy(
            wg_hbm.at[pl.ds(k * KW, KW), :], wg.at[k], w_sem.at[0, k]
        )
        loads["u", k] = pltpu.make_async_copy(
            wu_hbm.at[pl.ds(k * KW, KW), :], wu.at[k], w_sem.at[1, k]
        )
    for j in range(NC):
        loads["d", j] = pltpu.make_async_copy(
            wd_hbm.at[:, pl.ds(j * NW, NW)], wd.at[j], w_sem.at[2, j]
        )
    loads["a", 0] = pltpu.make_async_copy(ad_hbm, ad, w_sem.at[3, 0])
    for load in loads.values():
        load.start()
    own = []
    for k in range(KC):
        copy = pltpu.make_async_copy(
            tok_ref.at[:, pl.ds(k * KW, KW)], tokbuf.at[k, e, f], own_sem.at[k]
        )
        copy.start()
        own.append(copy)
    own_routes = pltpu.make_async_copy(routes_ref, routes_buf.at[e], own_sem.at[KC])
    own_routes.start()
    gram_buf[f] = lax.dot_general(
        up_ref[...], up_ref[...], (((1,), (1,)), ((), ())), preferred_element_type=jnp.float32
    )

    barrier = pltpu.get_barrier_semaphore()
    for d in range(1, F):
        pl.semaphore_signal(
            barrier, inc=1, device_id={"ffn": lax.rem(f + d, F)}, device_id_type=MESH
        )
    for d in range(1, E):
        pl.semaphore_signal(
            barrier, inc=1, device_id={"expert": lax.rem(e + d, E)}, device_id_type=MESH
        )
    pl.semaphore_wait(barrier, F + E - 2)

    sent = []

    def send(src, dst, send_sem, recv_sem, device):
        copy = pltpu.make_async_remote_copy(
            src_ref=src, dst_ref=dst, send_sem=send_sem, recv_sem=recv_sem,
            device_id=device, device_id_type=MESH,
        )
        copy.start()
        sent.append(copy)

    def receive(dst, send_sem, recv_sem, device):
        pltpu.make_async_remote_copy(
            src_ref=dst, dst_ref=dst, send_sem=send_sem, recv_sem=recv_sem,
            device_id=device, device_id_type=MESH,
        ).wait_recv()

    def ffn_to(d):
        return {"ffn": lax.rem(f + d, F)}

    def ffn_from(d):
        return lax.rem(f + F - d, F)

    def x_to(d):
        return lax.rem(x + d, X)

    def x_from(d):
        return lax.rem(x + X - d, X)

    for k in range(KC):
        for d in range(1, F):
            send(
                tok_ref.at[:, pl.ds(k * KW, KW)], tokbuf.at[k, e, f],
                tf_send.at[k, d], tf_recv.at[k, d], ffn_to(d),
            )
    for d in range(1, E):
        send(
            routes_ref, routes_buf.at[e], rt_send.at[d], rt_recv.at[d],
            {"expert": lax.rem(e + d, E)},
        )
    for d in range(1, F):
        send(gram_buf.at[f], gram_buf.at[f], gr_send.at[d], gr_recv.at[d], ffn_to(d))

    def forward_client(k):
        own[k].wait()
        for d in range(1, F):
            receive(
                tokbuf.at[k, e, ffn_from(d)], tf_send.at[k, d], tf_recv.at[k, d], ffn_to(d)
            )
        for d in range(1, X):
            send(
                tokbuf.at[k, e], tokbuf.at[k, e], tx_send.at[k, d], tx_recv.at[k, d],
                {"expert": x_to(d) * CORES + core},
            )
        send(
            tokbuf.at[k, e], tokbuf.at[k, e], tc_send.at[k, 0], tc_recv.at[k, 0],
            {"expert": mate},
        )

    def forward_x(k):
        for d in range(1, X):
            block = x_from(d) * CORES + core
            receive(
                tokbuf.at[k, block], tx_send.at[k, d], tx_recv.at[k, d], {"expert": block}
            )
            send(
                tokbuf.at[k, block], tokbuf.at[k, block], tc_send.at[k, d], tc_recv.at[k, d],
                {"expert": mate},
            )

    FT = tile_of(FFD)

    def expand(k):
        for d in range(X):
            block = x_from(d) * CORES + (CORES - 1 - core)
            receive(
                tokbuf.at[k, block], tc_send.at[k, d], tc_recv.at[k, d], {"expert": mate}
            )

        def compact(c, carry):
            rows = jnp.concatenate(
                [tokbuf[k, c, i].astype(jnp.float32) for i in range(F)], axis=0
            ).astype(jnp.bfloat16)
            tokc[k, pl.ds(pl.multiple_of(c * t, t), t), :] = rows
            return carry

        lax.fori_loop(0, E, compact, 0)
        loads["g", k].wait()
        loads["u", k].wait()

        def hidden_tile(i, carry):
            cols = pl.ds(pl.multiple_of(i * FT, FT), FT)
            g = jnp.dot(tokc[k], wg[k, :, cols], preferred_element_type=jnp.float32)
            u = jnp.dot(tokc[k], wu[k, :, cols], preferred_element_type=jnp.float32)
            if k > 0:
                g = gate_acc[:, cols] + g
                u = up_acc[:, cols] + u
            if k < KC - 1:
                gate_acc[:, cols] = g
                up_acc[:, cols] = u
            else:
                hid[:, cols] = (g / (1.0 + jnp.exp(-g)) * u).astype(jnp.bfloat16)
            return carry

        lax.fori_loop(0, FFD // FT, hidden_tile, 0)
        part = jnp.dot(
            tokc[k], router_ref[pl.ds(k * KW, KW), :], preferred_element_type=jnp.float32
        )
        logit_acc[...] = part if k == 0 else logit_acc[...] + part

    for step in range(KC + 2):
        if step < KC:
            forward_client(step)
        if 0 <= step - 1 < KC:
            forward_x(step - 1)
        if 0 <= step - 2:
            expand(step - 2)

    own_routes.wait()
    for d in range(1, E):
        receive(
            routes_buf.at[lax.rem(e + E - d, E)], rt_send.at[d], rt_recv.at[d],
            {"expert": lax.rem(e + d, E)},
        )
    routed = routes_buf[...].reshape(T, 2)
    logits = logit_acc[...]
    expert_ids = lax.broadcasted_iota(jnp.int32, (T, E), 1)
    first, second = routed[:, 0:1], routed[:, 1:2]
    picked_first = jnp.sum(jnp.where(expert_ids == first, logits, 0.0), axis=1, keepdims=True)
    picked_second = jnp.sum(jnp.where(expert_ids == second, logits, 0.0), axis=1, keepdims=True)
    weight_first = 1.0 / (1.0 + jnp.exp(picked_second - picked_first))
    share = jnp.where(first == e, weight_first, 0.0) + jnp.where(
        second == e, 1.0 - weight_first, 0.0
    )

    NT = tile_of(NW, (256, 128))

    def down(j):
        loads["d", j].wait()
        for n in range(NW // NT):
            value = jnp.dot(
                hid[...], wd[j, :, n * NT:(n + 1) * NT], preferred_element_type=jnp.float32
            )
            value = (value * share).astype(jnp.bfloat16)
            for c in range(E):
                for q in range(NT // CW):
                    sbuf[j, c % CORES, c // CORES, n * (NT // CW) + q] = value[
                        c * t:(c + 1) * t, q * CW:(q + 1) * CW
                    ]
        send(
            sbuf.at[j, CORES - 1 - core], r1.at[j], a_send.at[j], a_recv.at[j],
            {"expert": mate},
        )

    def add_mate(j):
        receive(r1.at[j], a_send.at[j], a_recv.at[j], {"expert": mate})
        for d in range(1, X + 1):
            to = x_to(d)
            s2[j, to] = (
                sbuf[j, core, to].astype(jnp.float32) + r1[j, to].astype(jnp.float32)
            ).astype(jnp.bfloat16)
            if d < X:
                send(
                    s2.at[j, to], r2.at[j, d], b_send.at[j, d], b_recv.at[j, d],
                    {"expert": to * CORES + core},
                )

    def add_x(j):
        total = s2[j, x].astype(jnp.float32)
        for d in range(1, X):
            receive(
                r2.at[j, d], b_send.at[j, d], b_recv.at[j, d],
                {"expert": x_from(d) * CORES + core},
            )
            total = total + r2[j, d].astype(jnp.float32)
        s3[j] = total.astype(jnp.bfloat16)
        for d in range(1, F):
            send(
                s3.at[j, lax.rem(f + d, F)], r3.at[j, d], c_send.at[j, d], c_recv.at[j, d],
                ffn_to(d),
            )

    def add_ffn(j):
        total = s3[j, f].astype(jnp.float32)
        for d in range(1, F):
            receive(r3.at[j, d], c_send.at[j, d], c_recv.at[j, d], ffn_to(d))
            total = total + r3[j, d].astype(jnp.float32)
        start = j * NW
        column = pl.multiple_of(lax.rem(start, KW) + f * CW, CW)
        rows = pl.ds(pl.multiple_of(e * t, t), t)
        if NW <= KW:
            mine = tokc[start // KW, rows, pl.ds(column, CW)]
        else:
            place = start + f * CW
            mine = tokc[place // KW, rows, pl.ds(pl.multiple_of(lax.rem(place, KW), CW), CW)]
        lbuf[j, f] = (mine.astype(jnp.float32) + total).astype(jnp.bfloat16)
        for d in range(1, F):
            send(lbuf.at[j, f], lbuf.at[j, f], d_send.at[j, d], d_recv.at[j, d], ffn_to(d))

    for step in range(NC + 5):
        if step < NC:
            down(step)
        if 0 <= step - 1 < NC:
            add_mate(step - 1)
        if 0 <= step - 3 < NC:
            add_x(step - 3)
        if 0 <= step - 5 < NC:
            add_ffn(step - 5)

    for d in range(1, F):
        receive(gram_buf.at[ffn_from(d)], gr_send.at[d], gr_recv.at[d], ffn_to(d))
    whole_gram = jnp.sum(gram_buf[...], axis=0)
    loads["a", 0].wait()
    layer_gram = jnp.zeros((t, t), jnp.float32)
    adapted = jnp.zeros((t, cd), jnp.float32)
    for j in range(NC):
        for d in range(1, F):
            receive(lbuf.at[j, ffn_from(d)], d_send.at[j, d], d_recv.at[j, d], ffn_to(d))
        block = jnp.concatenate([lbuf[j, i] for i in range(F)], axis=1)
        layer_ref[:, j * NW:(j + 1) * NW] = block
        layer_gram = layer_gram + lax.dot_general(
            block, block, (((1,), (1,)), ((), ())), preferred_element_type=jnp.float32
        )
        adapted = adapted + jnp.dot(
            block, ad[j * NW:(j + 1) * NW, :], preferred_element_type=jnp.float32
        )
    own_cols = layer_ref[:, pl.ds(pl.multiple_of(f * cd, cd), cd)]
    adapted_ref[...] = (own_cols.astype(jnp.float32) + adapted).astype(jnp.bfloat16)
    squared = jnp.sum(
        jnp.sum(layer_gram * whole_gram, axis=1, keepdims=True), axis=0, keepdims=True
    )
    limit = bound_ref[0]
    norm = jnp.sqrt(squared)
    factor_ref[...] = jnp.broadcast_to(limit / jnp.maximum(norm, limit), factor_ref.shape)
    for copy in sent:
        copy.wait_send()


def per_device(tokens, routes, router, w_gate, w_up, w_down, adapter, upstream, bound):
    E = lax.axis_size("expert")
    F = lax.axis_size("ffn")
    _, tl, D = tokens.shape
    t = routes.shape[1]
    FFD = w_gate.shape[2]
    cd = adapter.shape[2]
    KC = 4
    NC = max(1, min(4, D // (128 * F)))
    X, T, KW, NW = E // CORES, E * t, D // KC, D // NC
    CW = NW // F
    bf16, f32 = jnp.bfloat16, jnp.float32
    dma = pltpu.SemaphoreType.DMA
    vmem = pl.BlockSpec(memory_space=pltpu.VMEM)
    hbm = pl.BlockSpec(memory_space=pl.ANY)
    scratch = [
        pltpu.VMEM((KC, KW, FFD), bf16),
        pltpu.VMEM((KC, KW, FFD), bf16),
        pltpu.VMEM((NC, FFD, NW), bf16),
        pltpu.VMEM((D, cd), bf16),
        pltpu.VMEM((KC, E, F, tl, KW), bf16),
        pltpu.VMEM((KC, T, KW), bf16),
        pltpu.VMEM((T, FFD), f32),
        pltpu.VMEM((T, FFD), f32),
        pltpu.VMEM((T, FFD), bf16),
        pltpu.VMEM((T, E), f32),
        pltpu.VMEM((E, t, 2), jnp.int32),
        pltpu.VMEM((F, t, t), f32),
        pltpu.VMEM((NC, CORES, X, F, t, CW), bf16),
        pltpu.VMEM((NC, X, F, t, CW), bf16),
        pltpu.VMEM((NC, X, F, t, CW), bf16),
        pltpu.VMEM((NC, X, F, t, CW), bf16),
        pltpu.VMEM((NC, F, t, CW), bf16),
        pltpu.VMEM((NC, F, t, CW), bf16),
        pltpu.VMEM((NC, F, t, CW), bf16),
        dma((4, max(KC, NC))),
        dma((KC + 1,)),
        dma((E,)), dma((E,)),
        dma((F,)), dma((F,)),
        dma((KC, F)), dma((KC, F)),
        dma((KC, X)), dma((KC, X)),
        dma((KC, X)), dma((KC, X)),
        dma((NC,)), dma((NC,)),
        dma((NC, X)), dma((NC, X)),
        dma((NC, F)), dma((NC, F)),
        dma((NC, F)), dma((NC, F)),
    ]
    layer_out, adapted, factor = pl.pallas_call(
        functools.partial(layer_kernel, (E, F, KC, NC, D, FFD, t, tl, cd)),
        out_shape=(
            jax.ShapeDtypeStruct((t, D), bf16),
            jax.ShapeDtypeStruct((t, cd), bf16),
            jax.ShapeDtypeStruct((8, 128), f32),
        ),
        in_specs=[
            vmem, vmem, vmem, hbm, hbm, hbm, hbm, vmem,
            pl.BlockSpec(memory_space=pltpu.SMEM),
        ],
        out_specs=(vmem, vmem, vmem),
        scratch_shapes=scratch,
        compiler_params=pltpu.CompilerParams(
            collective_id=0, has_side_effects=True, vmem_limit_bytes=66 * 1000 * 1000
        ),
    )(
        tokens[0], routes[0], router, w_gate[0], w_up[0], w_down[0], adapter[0],
        upstream[0], bound,
    )
    adapter_grad = lax.dot_general(
        layer_out, upstream[0], (((0,), (0,)), ((), ())), preferred_element_type=jnp.float32
    )
    clipped = (adapter_grad * factor[0, 0]).astype(jnp.bfloat16)
    return (adapted[None], clipped[None])


def solution(mesh):
    in_specs = (
        P("expert", "ffn", None),
        P("expert", None, None),
        P(),
        P("expert", None, "ffn"),
        P("expert", None, "ffn"),
        P("expert", "ffn", None),
        P("expert", None, "ffn"),
        P("expert", None, "ffn"),
        P("expert"),
    )
    out_specs = (P("expert", None, "ffn"), P("expert", None, "ffn"))
    return jax.shard_map(
        per_device, mesh=mesh, in_specs=in_specs, out_specs=out_specs, check_vma=False
    )
```

```python
import functools

import jax
import jax.numpy as jnp
from jax import lax
from jax.experimental import pallas as pl
from jax.experimental.pallas import tpu as pltpu
from jax.sharding import PartitionSpec as P

MESH = pl.DeviceIdType.MESH
CORES = 2


def tile_of(size, choices=(512, 384, 256, 128)):
    for width in choices:
        if size % width == 0:
            return width
    return size


def layer_kernel(
    dims,
    tok_ref, routes_ref, router_ref, wg_hbm, wu_hbm, wd_hbm, ad_hbm, up_ref, bound_ref,
    layer_ref, adapted_ref, factor_ref,
    wg, wu, wd, ad, tokbuf, tokc, gate_acc, up_acc, hid, logit_acc, routes_buf, gram_buf,
    sbuf, r1, s2, r2, s3, r3, lbuf,
    w_sem, own_sem, rt_send, rt_recv, gr_send, gr_recv, tf_send, tf_recv, tx_send, tx_recv,
    tc_send, tc_recv, a_send, a_recv, b_send, b_recv, c_send, c_recv, d_send, d_recv,
):
    E, F, KC, NC, D, FFD, t, tl, cd = dims
    X = E // CORES
    T = E * t
    KW = D // KC
    NW = D // NC
    CW = NW // F
    e = lax.axis_index("expert")
    f = lax.axis_index("ffn")
    x, core = e // CORES, lax.rem(e, CORES)
    mate = x * CORES + (CORES - 1 - core)

    loads = {}
    for k in range(KC):
        loads["g", k] = pltpu.make_async_copy(
            wg_hbm.at[pl.ds(k * KW, KW), :], wg.at[k], w_sem.at[0, k]
        )
        loads["u", k] = pltpu.make_async_copy(
            wu_hbm.at[pl.ds(k * KW, KW), :], wu.at[k], w_sem.at[1, k]
        )
    for j in range(NC):
        loads["d", j] = pltpu.make_async_copy(
            wd_hbm.at[:, pl.ds(j * NW, NW)], wd.at[j], w_sem.at[2, j]
        )
    loads["a", 0] = pltpu.make_async_copy(ad_hbm, ad, w_sem.at[3, 0])
    for load in loads.values():
        load.start()
    own = []
    for k in range(KC):
        copy = pltpu.make_async_copy(
            tok_ref.at[:, pl.ds(k * KW, KW)], tokbuf.at[k, e, f], own_sem.at[k]
        )
        copy.start()
        own.append(copy)
    own_routes = pltpu.make_async_copy(routes_ref, routes_buf.at[e], own_sem.at[KC])
    own_routes.start()
    gram_buf[f] = lax.dot_general(
        up_ref[...], up_ref[...], (((1,), (1,)), ((), ())), preferred_element_type=jnp.float32
    )

    barrier = pltpu.get_barrier_semaphore()
    for d in range(1, F):
        pl.semaphore_signal(
            barrier, inc=1, device_id={"ffn": lax.rem(f + d, F)}, device_id_type=MESH
        )
    for d in range(1, E):
        pl.semaphore_signal(
            barrier, inc=1, device_id={"expert": lax.rem(e + d, E)}, device_id_type=MESH
        )
    pl.semaphore_wait(barrier, F + E - 2)

    sent = []

    def send(src, dst, send_sem, recv_sem, device):
        copy = pltpu.make_async_remote_copy(
            src_ref=src, dst_ref=dst, send_sem=send_sem, recv_sem=recv_sem,
            device_id=device, device_id_type=MESH,
        )
        copy.start()
        sent.append(copy)

    def receive(dst, send_sem, recv_sem, device):
        pltpu.make_async_remote_copy(
            src_ref=dst, dst_ref=dst, send_sem=send_sem, recv_sem=recv_sem,
            device_id=device, device_id_type=MESH,
        ).wait_recv()

    def ffn_to(d):
        return {"ffn": lax.rem(f + d, F)}

    def ffn_from(d):
        return lax.rem(f + F - d, F)

    def x_to(d):
        return lax.rem(x + d, X)

    def x_from(d):
        return lax.rem(x + X - d, X)

    for k in range(KC):
        for d in range(1, F):
            send(
                tok_ref.at[:, pl.ds(k * KW, KW)], tokbuf.at[k, e, f],
                tf_send.at[k, d], tf_recv.at[k, d], ffn_to(d),
            )
    for d in range(1, E):
        send(
            routes_ref, routes_buf.at[e], rt_send.at[d], rt_recv.at[d],
            {"expert": lax.rem(e + d, E)},
        )
    for d in range(1, F):
        send(gram_buf.at[f], gram_buf.at[f], gr_send.at[d], gr_recv.at[d], ffn_to(d))

    def forward_client(k):
        own[k].wait()
        for d in range(1, F):
            receive(
                tokbuf.at[k, e, ffn_from(d)], tf_send.at[k, d], tf_recv.at[k, d], ffn_to(d)
            )
        for d in range(1, X):
            send(
                tokbuf.at[k, e], tokbuf.at[k, e], tx_send.at[k, d], tx_recv.at[k, d],
                {"expert": x_to(d) * CORES + core},
            )
        send(
            tokbuf.at[k, e], tokbuf.at[k, e], tc_send.at[k, 0], tc_recv.at[k, 0],
            {"expert": mate},
        )

    def forward_x(k):
        for d in range(1, X):
            block = x_from(d) * CORES + core
            receive(
                tokbuf.at[k, block], tx_send.at[k, d], tx_recv.at[k, d], {"expert": block}
            )
            send(
                tokbuf.at[k, block], tokbuf.at[k, block], tc_send.at[k, d], tc_recv.at[k, d],
                {"expert": mate},
            )

    FT = tile_of(FFD)

    def expand(k):
        for d in range(X):
            block = x_from(d) * CORES + (CORES - 1 - core)
            receive(
                tokbuf.at[k, block], tc_send.at[k, d], tc_recv.at[k, d], {"expert": mate}
            )

        def compact(c, carry):
            rows = jnp.concatenate(
                [tokbuf[k, c, i].astype(jnp.float32) for i in range(F)], axis=0
            ).astype(jnp.bfloat16)
            tokc[k, pl.ds(pl.multiple_of(c * t, t), t), :] = rows
            return carry

        lax.fori_loop(0, E, compact, 0)
        loads["g", k].wait()
        loads["u", k].wait()

        def hidden_tile(i, carry):
            cols = pl.ds(pl.multiple_of(i * FT, FT), FT)
            g = jnp.dot(tokc[k], wg[k, :, cols], preferred_element_type=jnp.float32)
            u = jnp.dot(tokc[k], wu[k, :, cols], preferred_element_type=jnp.float32)
            if k > 0:
                g = gate_acc[:, cols] + g
                u = up_acc[:, cols] + u
            if k < KC - 1:
                gate_acc[:, cols] = g
                up_acc[:, cols] = u
            else:
                hid[:, cols] = (g / (1.0 + jnp.exp(-g)) * u).astype(jnp.bfloat16)
            return carry

        lax.fori_loop(0, FFD // FT, hidden_tile, 0)
        part = lax.dot_general(
            tokc[k], router_ref[:, pl.ds(k * KW, KW)], (((1,), (1,)), ((), ())),
            preferred_element_type=jnp.float32,
        )
        logit_acc[...] = part if k == 0 else logit_acc[...] + part

    for step in range(KC + 2):
        if step < KC:
            forward_client(step)
        if 0 <= step - 1 < KC:
            forward_x(step - 1)
        if 0 <= step - 2:
            expand(step - 2)

    own_routes.wait()
    for d in range(1, E):
        receive(
            routes_buf.at[lax.rem(e + E - d, E)], rt_send.at[d], rt_recv.at[d],
            {"expert": lax.rem(e + d, E)},
        )
    diagonal = lax.broadcasted_iota(jnp.int32, (t, t), 0) == lax.broadcasted_iota(
        jnp.int32, (t, t), 1
    )

    def choice(k):
        named = [routes_buf[c][k:k + 1, :].astype(jnp.float32) for c in range(E)]
        return jnp.concatenate(
            [jnp.sum(jnp.where(diagonal, row, 0.0), axis=1, keepdims=True) for row in named],
            axis=0,
        ).astype(jnp.int32)

    first, second = choice(0), choice(1)
    logits = logit_acc[...]
    expert_ids = lax.broadcasted_iota(jnp.int32, (T, E), 1)
    picked_first = jnp.sum(jnp.where(expert_ids == first, logits, 0.0), axis=1, keepdims=True)
    picked_second = jnp.sum(jnp.where(expert_ids == second, logits, 0.0), axis=1, keepdims=True)
    weight_first = 1.0 / (1.0 + jnp.exp(picked_second - picked_first))
    share = jnp.where(first == e, weight_first, 0.0) + jnp.where(
        second == e, 1.0 - weight_first, 0.0
    )

    NT = tile_of(NW, (256, 128))

    def down(j):
        loads["d", j].wait()
        for n in range(NW // NT):
            value = jnp.dot(
                hid[...], wd[j, :, n * NT:(n + 1) * NT], preferred_element_type=jnp.float32
            )
            value = (value * share).astype(jnp.bfloat16)
            for c in range(E):
                for q in range(NT // CW):
                    sbuf[j, c % CORES, c // CORES, n * (NT // CW) + q] = value[
                        c * t:(c + 1) * t, q * CW:(q + 1) * CW
                    ]
        send(
            sbuf.at[j, CORES - 1 - core], r1.at[j], a_send.at[j], a_recv.at[j],
            {"expert": mate},
        )

    def add_mate(j):
        receive(r1.at[j], a_send.at[j], a_recv.at[j], {"expert": mate})
        for d in range(1, X + 1):
            to = x_to(d)
            s2[j, to] = (
                sbuf[j, core, to].astype(jnp.float32) + r1[j, to].astype(jnp.float32)
            ).astype(jnp.bfloat16)
            if d < X:
                send(
                    s2.at[j, to], r2.at[j, d], b_send.at[j, d], b_recv.at[j, d],
                    {"expert": to * CORES + core},
                )

    def add_x(j):
        total = s2[j, x].astype(jnp.float32)
        for d in range(1, X):
            receive(
                r2.at[j, d], b_send.at[j, d], b_recv.at[j, d],
                {"expert": x_from(d) * CORES + core},
            )
            total = total + r2[j, d].astype(jnp.float32)
        s3[j] = total.astype(jnp.bfloat16)
        for d in range(1, F):
            send(
                s3.at[j, lax.rem(f + d, F)], r3.at[j, d], c_send.at[j, d], c_recv.at[j, d],
                ffn_to(d),
            )

    def add_ffn(j):
        total = s3[j, f].astype(jnp.float32)
        for d in range(1, F):
            receive(r3.at[j, d], c_send.at[j, d], c_recv.at[j, d], ffn_to(d))
            total = total + r3[j, d].astype(jnp.float32)
        start = j * NW
        column = pl.multiple_of(lax.rem(start, KW) + f * CW, CW)
        rows = pl.ds(pl.multiple_of(e * t, t), t)
        if NW <= KW:
            mine = tokc[start // KW, rows, pl.ds(column, CW)]
        else:
            place = start + f * CW
            mine = tokc[place // KW, rows, pl.ds(pl.multiple_of(lax.rem(place, KW), CW), CW)]
        lbuf[j, f] = (mine.astype(jnp.float32) + total).astype(jnp.bfloat16)
        for d in range(1, F):
            send(lbuf.at[j, f], lbuf.at[j, f], d_send.at[j, d], d_recv.at[j, d], ffn_to(d))

    for step in range(NC + 5):
        if step < NC:
            down(step)
        if 0 <= step - 1 < NC:
            add_mate(step - 1)
        if 0 <= step - 3 < NC:
            add_x(step - 3)
        if 0 <= step - 5 < NC:
            add_ffn(step - 5)

    for d in range(1, F):
        receive(gram_buf.at[ffn_from(d)], gr_send.at[d], gr_recv.at[d], ffn_to(d))
    whole_gram = jnp.sum(gram_buf[...], axis=0)
    loads["a", 0].wait()
    layer_gram = jnp.zeros((t, t), jnp.float32)
    adapted = jnp.zeros((t, cd), jnp.float32)
    for j in range(NC):
        for d in range(1, F):
            receive(lbuf.at[j, ffn_from(d)], d_send.at[j, d], d_recv.at[j, d], ffn_to(d))
        block = jnp.concatenate([lbuf[j, i] for i in range(F)], axis=1)
        layer_ref[:, j * NW:(j + 1) * NW] = block
        layer_gram = layer_gram + lax.dot_general(
            block, block, (((1,), (1,)), ((), ())), preferred_element_type=jnp.float32
        )
        adapted = adapted + jnp.dot(
            block, ad[j * NW:(j + 1) * NW, :], preferred_element_type=jnp.float32
        )
    own_cols = layer_ref[:, pl.ds(pl.multiple_of(f * cd, cd), cd)]
    adapted_ref[...] = (own_cols.astype(jnp.float32) + adapted).astype(jnp.bfloat16)
    squared = jnp.sum(
        jnp.sum(layer_gram * whole_gram, axis=1, keepdims=True), axis=0, keepdims=True
    )
    limit = bound_ref[0]
    norm = jnp.sqrt(squared)
    factor_ref[...] = jnp.broadcast_to(limit / jnp.maximum(norm, limit), factor_ref.shape)
    for copy in sent:
        copy.wait_send()


def grad_kernel(
    RB, layer_ref, up_ref, factor_ref, adapted_in, adapted_ref, clipped_hbm, blocks, sems
):
    factor = factor_ref[0:1, 0:1]
    copies = []
    for i in range(blocks.shape[0]):
        grad = lax.dot_general(
            layer_ref[:, i * RB:(i + 1) * RB], up_ref[...], (((0,), (0,)), ((), ())),
            preferred_element_type=jnp.float32,
        )
        blocks[i] = (grad * factor).astype(jnp.bfloat16)
        copy = pltpu.make_async_copy(
            blocks.at[i], clipped_hbm.at[pl.ds(i * RB, RB), :], sems.at[i]
        )
        copy.start()
        copies.append(copy)
    adapted_ref[...] = adapted_in[...]
    for copy in copies:
        copy.wait()


def per_device(tokens, routes, router, w_gate, w_up, w_down, adapter, upstream, bound):
    E = lax.axis_size("expert")
    F = lax.axis_size("ffn")
    _, tl, D = tokens.shape
    t = routes.shape[1]
    FFD = w_gate.shape[2]
    cd = adapter.shape[2]
    KC = 4
    NC = max(1, min(4, D // (128 * F)))
    X, T, KW, NW = E // CORES, E * t, D // KC, D // NC
    CW = NW // F
    bf16, f32 = jnp.bfloat16, jnp.float32
    dma = pltpu.SemaphoreType.DMA
    vmem = pl.BlockSpec(memory_space=pltpu.VMEM)
    hbm = pl.BlockSpec(memory_space=pl.ANY)
    scratch = [
        pltpu.VMEM((KC, KW, FFD), bf16),
        pltpu.VMEM((KC, KW, FFD), bf16),
        pltpu.VMEM((NC, FFD, NW), bf16),
        pltpu.VMEM((D, cd), bf16),
        pltpu.VMEM((KC, E, F, tl, KW), bf16),
        pltpu.VMEM((KC, T, KW), bf16),
        pltpu.VMEM((T, FFD), f32),
        pltpu.VMEM((T, FFD), f32),
        pltpu.VMEM((T, FFD), bf16),
        pltpu.VMEM((T, E), f32),
        pltpu.VMEM((E, 2, t), jnp.int32),
        pltpu.VMEM((F, t, t), f32),
        pltpu.VMEM((NC, CORES, X, F, t, CW), bf16),
        pltpu.VMEM((NC, X, F, t, CW), bf16),
        pltpu.VMEM((NC, X, F, t, CW), bf16),
        pltpu.VMEM((NC, X, F, t, CW), bf16),
        pltpu.VMEM((NC, F, t, CW), bf16),
        pltpu.VMEM((NC, F, t, CW), bf16),
        pltpu.VMEM((NC, F, t, CW), bf16),
        dma((4, max(KC, NC))),
        dma((KC + 1,)),
        dma((E,)), dma((E,)),
        dma((F,)), dma((F,)),
        dma((KC, F)), dma((KC, F)),
        dma((KC, X)), dma((KC, X)),
        dma((KC, X)), dma((KC, X)),
        dma((NC,)), dma((NC,)),
        dma((NC, X)), dma((NC, X)),
        dma((NC, F)), dma((NC, F)),
        dma((NC, F)), dma((NC, F)),
    ]
    layer_out, adapted, factor = pl.pallas_call(
        functools.partial(layer_kernel, (E, F, KC, NC, D, FFD, t, tl, cd)),
        out_shape=(
            jax.ShapeDtypeStruct((t, D), bf16),
            jax.ShapeDtypeStruct((t, cd), bf16),
            jax.ShapeDtypeStruct((8, 128), f32),
        ),
        in_specs=[
            vmem, vmem, vmem, hbm, hbm, hbm, hbm, vmem,
            pl.BlockSpec(memory_space=pltpu.SMEM),
        ],
        out_specs=(vmem, vmem, vmem),
        scratch_shapes=scratch,
        compiler_params=pltpu.CompilerParams(
            collective_id=0, has_side_effects=True, vmem_limit_bytes=63_500_000
        ),
    )(
        tokens[0], routes[0].T, router.T, w_gate[0], w_up[0], w_down[0], adapter[0],
        upstream[0], bound,
    )
    RB = D // 8
    adapted, clipped = pl.pallas_call(
        functools.partial(grad_kernel, RB),
        out_shape=(
            jax.ShapeDtypeStruct((t, cd), bf16),
            jax.ShapeDtypeStruct((D, cd), bf16),
        ),
        in_specs=[vmem, vmem, vmem, vmem],
        out_specs=(vmem, hbm),
        scratch_shapes=[pltpu.VMEM((D // RB, RB, cd), bf16), dma((D // RB,))],
    )(layer_out, upstream[0], factor, adapted)
    return (adapted[None], clipped[None])


def solution(mesh):
    in_specs = (
        P("expert", "ffn", None),
        P("expert", None, None),
        P(),
        P("expert", None, "ffn"),
        P("expert", None, "ffn"),
        P("expert", "ffn", None),
        P("expert", None, "ffn"),
        P("expert", None, "ffn"),
        P("expert"),
    )
    out_specs = (P("expert", None, "ffn"), P("expert", None, "ffn"))
    return jax.shard_map(
        per_device, mesh=mesh, in_specs=in_specs, out_specs=out_specs, check_vma=False
    )
```
